32 devices in a mesh: prow: 4 (over y, core), pcol: 8 (over z, x).
Axes of the slice: x: 2, y: 2, z: 4, core: 2. Of those that a mesh axis runs over, the one named last changes fastest.
Arguments:
- vectors: bfloat16 [512, 120064], P('pcol', 'prow'), may hold values from -6 to 6
- reflectors: bfloat16 [2, 256, 120064], P(None, 'pcol', 'prow'), may hold values from -6 to 6
- panel_factor: float32 [2, 256, 256], replicated, as said below
Outputs:
- band_vectors: bfloat16 [8, 64, 120064], P('pcol', 'prow')
The draws below stay inside these ranges and needn't reach their ends.
Inputs may be any that keep to these rules, and one draw needn't show every extreme that they name: `panel_factor`: upper triangular: zero below the diagonal; diagonal entries between 1 / 120064 and 3 / 120064.
All inputs are finite; a program needn't handle non-finite values.
Results may differ from the reference program's by a relative error of at most 0.0095.
Values may be sent and summed in bfloat16 or wider, within the bound.
No kernel may reach another device: no remote copies, remote signals or barrier semaphores. Data moves between devices by JAX's collectives and lax.ppermute only.
A program may use at most 192 MiB of HBM per device.

```python
import jax
import jax.numpy as jnp
from jax import lax

ORDER = 120064
PANEL = 256
PANELS = 2
COLS_DEV = 64
NEV = 512
N_PCOL = 8


def draw_panel_factor(key, part):
    first_key, second_key = jax.random.split(jax.random.fold_in(key, 7))
    shape = (PANELS, PANEL, PANEL)
    upper_part = jax.random.normal(first_key, shape, jnp.float32) * (0.6 / ORDER)
    diag_part = jax.random.uniform(second_key, (PANELS, PANEL), jnp.float32, 1.0, 3.0) / ORDER
    row_ids = lax.broadcasted_iota(jnp.int32, shape, 1)
    col_ids = lax.broadcasted_iota(jnp.int32, shape, 2)
    result = jnp.where(col_ids > row_ids, upper_part, 0.0)
    result = result + jnp.where(col_ids == row_ids, diag_part[:, :, None], 0.0)
    return result.astype(jnp.float32)


def shard_levels(own_key, dims, pieces, low, top_value):
    factor_of = 1.0
    for position, blocks in pieces:
        steps = jax.random.uniform(jax.random.fold_in(jax.random.fold_in(own_key, 6), position), (blocks,), jnp.float32, low / len(pieces), top_value / len(pieces))
        factor_of = factor_of * jnp.repeat(jnp.exp(steps), dims[position] // blocks).reshape((-1,) + (1,) * (len(dims) - 1 - position))
    return factor_of


def scatter_about(rng, shape, deviation, most, cuts=(), dtype=jnp.bfloat16):
    entries = deviation * jax.random.normal(rng, shape, jnp.float32)
    if cuts:
        entries = entries * shard_levels(rng, shape, cuts, -0.22, 0.18)
    return jnp.clip(entries, -most, most).astype(dtype)


def setup_inputs(seed: int = 0) -> dict:
    streams_of = jax.random.split(jax.random.key(seed), 4)
    vectors = scatter_about(streams_of[0], (NEV, ORDER), 1.0, 6.0, ((0, 8), (1, 4)))
    reflectors = scatter_about(streams_of[1], (PANELS, PANEL, ORDER), 1.0, 6.0, ((1, 8), (2, 4)))
    panel_factor = draw_panel_factor(jax.random.fold_in(streams_of[3], 71), 0)
    return dict(vectors=vectors, reflectors=reflectors, panel_factor=panel_factor)


def apply_panel(current, panel, factor):
    projected = lax.dot_general(current, panel, (((1,), (1,)), ((), ())), preferred_element_type=jnp.float32)
    scaled = lax.dot_general(projected, factor, (((1,), (1,)), ((), ())), precision=lax.Precision.HIGHEST, preferred_element_type=jnp.float32).astype(jnp.bfloat16)
    updated = current.astype(jnp.float32) - jnp.dot(scaled, panel, preferred_element_type=jnp.float32)
    return updated.astype(jnp.bfloat16)


def reference(vectors, reflectors, panel_factor):
    current = vectors
    for number in range(PANELS):
        current = apply_panel(current, reflectors[number], panel_factor[number])
    return current.reshape(N_PCOL, COLS_DEV, ORDER)
```

```python
import functools

import jax
import jax.numpy as jnp
from jax import lax
from jax.experimental import pallas as pl
from jax.experimental.pallas import tpu as pltpu
from jax.sharding import Mesh, PartitionSpec as P

LANES = 128
WIDEST = 16
INNER_SHARE = (0.36, 0.48)

F32 = jnp.float32
BF16 = jnp.bfloat16


def block_tiles(tiles):
    return max(size for size in range(1, WIDEST + 1) if tiles % size == 0)


def split_tiles(tiles):
    low, high = (round(tiles * share) for share in INNER_SHARE)
    choices = range(low, high + 1)
    inner = max(choices, key=lambda t: (min(block_tiles(t), block_tiles(tiles - t)), t))
    return tiles - inner, inner


def stacked(refs_of_piece):
    parts = []
    for terms in refs_of_piece:
        value = terms[0][0][terms[0][1]]
        for ref, lead in terms[1:]:
            value = value + ref[lead]
        parts.append(value)
    return jnp.concatenate(parts, axis=0)


def piece_operands(pieces):
    arrays, plan, seen = [], [], {}
    for terms in pieces:
        row = []
        for array, lead in terms:
            if id(array) not in seen:
                seen[id(array)] = len(arrays)
                arrays.append(array)
            row.append((seen[id(array)], lead))
        plan.append(row)
    return arrays, plan


def piece_specs(arrays, block):
    return [pl.BlockSpec((*a.shape[:2], block), lambda i: (0, 0, i)) for a in arrays]


def row_specs(arrays, block):
    return [pl.BlockSpec((a.shape[0], block), lambda i: (0, i)) for a in arrays]


def products(rows, pieces, name):
    width = rows[0].shape[1]
    block = block_tiles(width // LANES) * LANES
    arrays, plan = piece_operands(pieces)
    count, height = len(rows), rows[0].shape[0]
    total = sum(terms[0][0].shape[1] for terms in pieces)

    def kernel(*refs):
        row_refs, piece_refs, out = refs[:count], refs[count:-1], refs[-1]
        panel = stacked([[(piece_refs[k], lead) for k, lead in terms] for terms in plan])
        current = jnp.concatenate([r[...] for r in row_refs], axis=0)
        part = lax.dot_general(
            current, panel, (((1,), (1,)), ((), ())), preferred_element_type=F32
        ).reshape(count, height, total)

        @pl.when(pl.program_id(0) == 0)
        def _():
            out[...] = part

        @pl.when(pl.program_id(0) > 0)
        def _():
            out[...] += part

    moved = sum(a.size for a in (*rows, *arrays)) * 2
    return pl.pallas_call(
        kernel,
        grid=(width // block,),
        in_specs=row_specs(rows, block) + piece_specs(arrays, block),
        out_specs=pl.BlockSpec((count, height, total), lambda i: (0, 0, 0)),
        out_shape=jax.ShapeDtypeStruct((count, height, total), F32),
        cost_estimate=pl.CostEstimate(
            flops=2 * count * height * total * width, bytes_accessed=moved, transcendentals=0
        ),
        name=name,
    )(*rows, *arrays)


def updated(rows, scaled, pieces, name, swap=None):
    width = rows[0].shape[1]
    block = block_tiles(width // LANES) * LANES
    arrays, plan = piece_operands(pieces)
    count, height = len(rows), rows[0].shape[0]
    total = scaled.shape[-1]
    scalars = 0 if swap is None else 1

    def kernel(*refs):
        head, refs = refs[:scalars], refs[scalars:]
        row_refs, factor = refs[:count], refs[count]
        piece_refs, outs = refs[count + 1 : count + 1 + len(arrays)], refs[count + 1 + len(arrays) :]
        panel = stacked([[(piece_refs[k], lead) for k, lead in terms] for terms in plan])
        change = jnp.dot(
            factor[...].reshape(count * height, total), panel, preferred_element_type=F32
        )
        for k in range(count):
            fresh = row_refs[k][...].astype(F32) - change[k * height : (k + 1) * height]
            if scalars:
                outs[k // 2][head[0][0] ^ (k % 2)] = fresh.astype(BF16)
            else:
                outs[k][...] = fresh.astype(BF16)

    moved = (sum(a.size for a in (*rows, *arrays)) + count * height * width) * 2
    cost = pl.CostEstimate(
        flops=2 * count * height * total * width, bytes_accessed=moved, transcendentals=0
    )
    in_specs = row_specs(rows, block)
    in_specs.append(pl.BlockSpec((count, height, total), lambda i: (0, 0, 0)))
    in_specs += piece_specs(arrays, block)
    if scalars:
        in_specs.insert(0, pl.BlockSpec(memory_space=pltpu.SMEM))
        out_specs = [pl.BlockSpec((2, height, block), lambda i: (0, 0, i))] * (count // 2)
        out_shape = [jax.ShapeDtypeStruct((2, height, width), BF16)] * (count // 2)
    else:
        out_specs = row_specs(rows, block)
        out_shape = [jax.ShapeDtypeStruct((height, width), BF16)] * count
    return pl.pallas_call(
        kernel,
        grid=(width // block,),
        in_specs=in_specs,
        out_specs=out_specs,
        out_shape=out_shape,
        cost_estimate=cost,
        name=name,
    )(*([swap] if scalars else []), *rows, scaled, *arrays)


def joined(outer, inner, n_prow, columns, half):
    height = outer.shape[1]
    wide = outer.shape[2]

    def kernel(outer_ref, inner_ref, out):
        for r in range(n_prow):
            pieces = []
            for k in range(2):
                pieces.append(outer_ref[k * n_prow + r])
                left = min(inner.shape[2], columns - k * half - wide)
                pieces.append(inner_ref[k * n_prow + r][:, :left])
            out[0, :, r * columns : (r + 1) * columns] = jnp.concatenate(pieces, axis=1)

    return pl.pallas_call(
        kernel,
        out_shape=jax.ShapeDtypeStruct((1, height, n_prow * columns), BF16),
        cost_estimate=pl.CostEstimate(
            flops=0, bytes_accessed=4 * height * n_prow * columns, transcendentals=0
        ),
        name="joined",
    )(outer, inner)


def body(vectors, reflectors, panel_factor, *, n_prow, n_line):
    line = ("zh", "zl")
    n_panels, height, columns = reflectors.shape
    tiles = pl.cdiv(pl.cdiv(columns, LANES), 2)
    half = tiles * LANES
    wide, narrow = (t * LANES for t in split_tiles(tiles))
    spans = ((0, wide), (wide, half))
    z = lax.axis_index(line)
    zl = lax.axis_index("zl")
    x = lax.axis_index("x")
    is_inner = (z > 0) & (z < n_line - 1)
    swap_pairs = [(0, 1), (1, 0)]
    across = functools.partial(lax.ppermute, axis_name="x", perm=swap_pairs)

    def choose(array, span, first):
        lo, hi = span
        left = array[:, lo:hi]
        right = array[:, half + lo : min(half + hi, columns)]
        right = jnp.pad(right, ((0, 0), (0, hi - lo - right.shape[1])))
        return jnp.where(first, left, right)

    def kept(array, span):
        return choose(array, span, x == 0)

    def given(array, span):
        return choose(array, span, x == 1)

    def hop(array, step, upward, last):
        pairs = [(i, i + 1) for i in range(step - 1, last)]
        if not upward:
            pairs = [(n_line - 1 - a, n_line - 1 - b) for a, b in pairs]
        return lax.ppermute(array, line, pairs)

    last = (n_line - 1, n_line - 2)
    ends = [(0, 1), (n_line - 1, n_line - 2)]

    class Stream:
        def __init__(self, own):
            self.got = [{0: [array]} for array in own]
            self.at = [[(array, array)] for array in own]

        def step(self, cls, step):
            if step > last[cls]:
                return
            up, down = self.at[cls][step - 1]
            up = hop(up, step, True, last[cls])
            down = hop(down, step, False, last[cls])
            self.at[cls].append((up, down))
            self.got[cls].setdefault(step % n_line, []).append(up)
            self.got[cls].setdefault((n_line - step) % n_line, []).append(down)

    own = [[kept(reflectors[0], s)[None] for s in spans]]
    sent = [[given(reflectors[0], s)[None] for s in spans]]
    other = [[across(a) for a in sent[0]]]
    own_rows = [kept(vectors, s) for s in spans]
    other_rows = [across(given(vectors, s)) for s in spans]
    for p in range(1, n_panels):
        own.append([kept(reflectors[p], s)[None] for s in spans])
        other.append([across(given(reflectors[p], s)[None]) for s in spans])
    end_rows = [lax.ppermute(a, line, ends) for a in (own_rows[1], other_rows[1])]

    position = jnp.arange(n_panels * 0 + 2 * n_line * height)
    side, rest = position // (n_line * height), position % (n_line * height)
    back, item = rest // height, rest % height
    source = (((z - back) % n_line) * 2 + (x ^ side)) * height + item
    chosen = (source[:, None] == position[None, :]).astype(F32)
    exact = functools.partial(
        lax.dot_general, precision=lax.Precision.HIGHEST, preferred_element_type=F32
    )
    factors = [
        exact(
            exact(chosen, panel_factor[p], (((1,), (0,)), ((), ()))),
            chosen,
            (((1,), (1,)), ((), ())),
        )
        for p in range(n_panels)
    ]

    def total(outer, inner):
        n_lanes = outer.shape[2]
        inner = jnp.where(is_inner, inner, 0.0)
        value = jnp.concatenate([outer + inner[:2], inner[2:]], axis=0)
        for bit in (1, 2, 4, 8):
            if bit < n_prow:
                pairs = [(i, i ^ bit) for i in range(n_prow)]
                value = value + lax.ppermute(value.astype(BF16), "prow", pairs).astype(F32)
        mirrored = across(value.astype(BF16)).astype(F32)
        mirrored = jnp.stack([mirrored[1], mirrored[0], mirrored[3], mirrored[2]])
        mirrored = jnp.concatenate(
            [mirrored[:, :, n_lanes // 2 :], mirrored[:, :, : n_lanes // 2]], axis=2
        )
        value = value + mirrored
        mine = jnp.where(is_inner, value[2:], value[:2])
        theirs = lax.ppermute(mine.astype(BF16), "zl", swap_pairs).astype(F32)
        theirs = theirs.reshape(2, -1, 2, n_lanes // 2)
        theirs = jnp.where(
            zl == 0, jnp.roll(theirs, -height, axis=3), jnp.roll(theirs, height, axis=3)
        )
        mine = mine + theirs.reshape(2, -1, n_lanes)
        return jnp.concatenate([jnp.where(is_inner, value[:2], mine), mine], axis=0)

    outer_rows = [own_rows[0], other_rows[0]]
    inner_rows = [own_rows[1], other_rows[1], *end_rows]
    for p in range(n_panels):
        if p == 0:
            streams = [Stream(own[p]), Stream(other[p])]
            leads = ((0, 0), (1, 0))
        else:
            both = [jnp.concatenate(pair, axis=0) for pair in zip(own[p], other[p])]
            streams = [Stream(both)]
            leads = ((0, 0), (0, 1))
        for step in range(1, n_line):
            for stream in streams:
                for cls in (0, 1):
                    stream.step(cls, step)
        pieces = [
            [
                [(array, lead) for array in streams[k].got[cls][back_steps]]
                for k, lead in leads
                for back_steps in range(n_line)
            ]
            for cls in (0, 1)
        ]
        sums = total(
            products(outer_rows, pieces[0], f"products_outer_{p}"),
            products(inner_rows, pieces[1], f"products_inner_{p}"),
        )
        n_rows = sums.shape[1]
        scaled = exact(
            sums.reshape(-1, sums.shape[2]), factors[p], (((1,), (1,)), ((), ()))
        ).astype(BF16).reshape(4, n_rows, -1)
        if p < n_panels - 1:
            outer_rows = updated(outer_rows, scaled[:2], pieces[0], f"update_outer_{p}")
            inner_rows = updated(inner_rows, scaled, pieces[1], f"update_inner_{p}")
        else:
            swap = x.reshape(1)
            inner_mine, inner_end = updated(
                inner_rows, scaled, pieces[1], f"update_inner_{p}", swap
            )
            inner_end = lax.ppermute(inner_end, line, [(b, a) for a, b in ends])
            (outer_mine,) = updated(outer_rows, scaled[:2], pieces[0], f"update_outer_{p}", swap)

    def to_owner(array):
        array = array.reshape(2 * n_prow, -1, array.shape[2])
        return lax.all_to_all(array, ("x", "prow"), 0, 0, tiled=True)

    outer_mine = to_owner(outer_mine)
    inner_mine = to_owner(jnp.where(is_inner, inner_mine, inner_end))
    return joined(outer_mine, inner_mine, n_prow, columns, half)


def solution(mesh):
    n_prow, n_pcol = (mesh.shape[axis] for axis in ("prow", "pcol"))
    n_line = n_pcol // 2
    devices = mesh.devices.reshape(n_prow, n_line // 2, 2, 2)
    grid = Mesh(devices, ("prow", "zh", "zl", "x"))
    pcol = ("zh", "zl", "x")
    placed = (P(pcol, "prow"), P(None, pcol, "prow"), P())
    return jax.shard_map(
        functools.partial(body, n_prow=n_prow, n_line=n_line),
        mesh=grid,
        in_specs=placed,
        out_specs=P(pcol, "prow", None),
        check_vma=False,
    )
```
